32 devices in a mesh: pair: 8 (over z, x), aux: 4 (over y, core).
Axes of the slice: x: 2, y: 2, z: 4, core: 2. Of those that a mesh axis runs over, the one named last changes fastest.
Arguments:
- panels: bfloat16 [16, 120, 9216], P('pair', None, 'aux'), may hold values from -1.5 to 1.5
- amplitudes: bfloat16 [16, 2, 120, 120], P('pair'), may hold values from -0.5 to 0.5
- drive: float32 [16, 2, 14400], P('pair', None, 'aux'), may hold values from -6 to 6
- pno_energy: float32 [16, 120], P('pair'), may hold values from 1 to 3
- occ_energy: float32 [32], replicated, may hold values from -2 to -0.5
- frequency: float32 [1], replicated, may hold values from 0.2 to 2
- pair_lmo: int32 [16, 2], replicated, may hold values from 0 to 31
- neighbours: int32 [16, 8], P('pair'), may hold values from 0 to 15
- pno_ranks: int32 [16], P('pair'), may hold values from 60 to 120
- fock_off: float32 [32, 32], replicated, may hold values from -1.8 to 1.8
Outputs:
- residual: float32 [16, 2, 14400], P('pair', None, 'aux')
The draws below stay inside these ranges and needn't reach their ends.
Inputs may be any that keep to these rules, and one draw needn't show every extreme that they name: `neighbours`: neighbour pairs; a pair may be listed more than once and may list itself. `pno_ranks`: rows of a pair's panel from its rank on are padding.
All inputs are finite; a program needn't handle non-finite values.
Results may differ from the reference program's by a relative error of at most 0.0033.
Values may be sent and summed in bfloat16 or wider, within the bound.
A program may use at most 128 MiB of HBM per device.

```python
import jax
import jax.numpy as jnp
from jax import lax

R = 120
AUX_DEV = 2304
AUX = 9216
PAIRS = 16
NBR = 8
NLMO = 32
RR = 14400
N_AUX = 4


def plant(values, rng, least, high):
    longest = values.shape.index(max(values.shape))
    spots = []
    for shift in (0, 1):
        where = [jax.random.randint(jax.random.fold_in(rng, axis), (), 0, length) for axis, length in enumerate(values.shape)]
        where[longest] = (where[longest] + shift) % values.shape[longest]
        spots.append(tuple(where))
    return values.at[spots[0]].set(least).at[spots[1]].set(high)


def levels(own_key, shape, pieces, least, largest):
    def one(axis_at, shards_of):
        draws = jax.random.uniform(jax.random.fold_in(jax.random.fold_in(own_key, 6), axis_at), (shards_of,), jnp.float32, least / len(pieces), largest / len(pieces))
        return jnp.repeat(jnp.exp(draws), shape[axis_at] // shards_of).reshape((-1,) + (1,) * (len(shape) - axis_at - 1))

    loudness = one(*pieces[0])
    for cut in pieces[1:]:
        loudness = loudness * one(*cut)
    return loudness


def bell_draw(rng, dims, width, reach, split=(), kind=jnp.bfloat16):
    entries = jax.random.normal(rng, dims, jnp.float32) * width
    if len(split) > 0:
        entries = levels(rng, dims, split, -0.22, 0.18) * entries
    return jnp.clip(entries, min=-reach, max=reach).astype(kind)


def setup_inputs(seed: int = 0) -> dict:
    splits = jax.random.split(jax.random.key(seed), 11)
    return {
        "panels": bell_draw(splits[0], (PAIRS, R, AUX), (AUX ** -0.25), 1.5, ((0, 8), (2, 4))),
        "amplitudes": bell_draw(splits[1], (PAIRS, 2, R, R), R ** -0.5, 0.5, ((0, 8),)),
        "drive": bell_draw(splits[2], (PAIRS, 2, RR), 1.0, 6.0, ((0, 8), (2, 4)), jnp.float32),
        "pno_energy": jnp.clip(1.0 + 2.0 * jax.random.uniform(splits[3], (PAIRS, R), jnp.float32) ** levels(splits[3], (PAIRS, R), ((0, 8),), -0.2, 0.2), 1.0, 3.0),
        "occ_energy": jnp.clip(jax.random.uniform(splits[4], (NLMO,), jnp.float32, -2.0, -0.5), -2.0, -0.5),
        "frequency": jnp.clip(jax.random.uniform(splits[5], (1,), jnp.float32, 0.2, 2.0), 0.2, 2.0),
        "pair_lmo": plant(jax.random.randint(splits[6], (PAIRS, 2), 0, NLMO), jax.random.fold_in(splits[6], 1), 0, NLMO - 1).astype(jnp.int32),
        "neighbours": plant(jax.random.randint(splits[7], (PAIRS, NBR), 0, PAIRS), jax.random.fold_in(splits[7], 1), 0, PAIRS - 1).astype(jnp.int32),
        "pno_ranks": plant(jax.random.randint(splits[8], (PAIRS,), R // 2, R + 1), jax.random.fold_in(splits[8], 1), R // 2, R).astype(jnp.int32),
        "fock_off": bell_draw(splits[9], (NLMO, NLMO), 0.3, 1.8, (), jnp.float32),
    }


def reference(panels, amplitudes, drive, pno_energy, occ_energy, frequency, pair_lmo, neighbours, pno_ranks, fock_off):
    rows_index = jnp.arange(R, dtype=jnp.int32)
    keep_rows = rows_index[None, :] < pno_ranks[:, None]
    masked = jnp.where(keep_rows[:, :, None], panels, jnp.zeros_like(panels))
    near_lmo = pair_lmo[neighbours]
    values = fock_off[pair_lmo[:, 0][:, None], near_lmo[:, :, 0]] + fock_off[pair_lmo[:, 1][:, None], near_lmo[:, :, 1]]
    onehot = (neighbours[:, :, None] == jnp.arange(PAIRS, dtype=jnp.int32)[None, None, :]).astype(jnp.float32)
    weights = jnp.sum(values[:, :, None] * onehot, axis=1).astype(jnp.bfloat16)
    weights_wide = weights.astype(jnp.float32)
    matrices = jnp.transpose(amplitudes, (0, 2, 1, 3)).reshape(PAIRS, R, 2 * R).astype(jnp.float32)

    def block_step(running_sum, block_index):
        start_col = (block_index * AUX_DEV).astype(jnp.int32)
        slab = lax.dynamic_slice_in_dim(masked, start_col, AUX_DEV, 2).astype(jnp.float32)
        projected = jnp.einsum('nra,nrc->nac', slab, matrices, precision=lax.Precision.HIGHEST).astype(jnp.bfloat16)
        projected = lax.optimization_barrier(projected).astype(jnp.float32)
        collected = jnp.einsum('pn,nac->pac', weights_wide, projected, precision=lax.Precision.HIGHEST).astype(jnp.bfloat16)
        collected = lax.optimization_barrier(collected).astype(jnp.float32)
        running_sum = running_sum + jnp.einsum('pra,pac->prc', slab, collected, precision=lax.Precision.HIGHEST)
        return running_sum, None

    start_sum = jnp.zeros((PAIRS, R, 2 * R), jnp.float32)
    coupled, unused_out = lax.scan(block_step, start_sum, jnp.arange(N_AUX, dtype=jnp.int32))
    coupled = jnp.transpose(coupled.reshape(PAIRS, R, 2, R), (0, 2, 1, 3))
    occ_pair = occ_energy[pair_lmo[:, 0]] + occ_energy[pair_lmo[:, 1]]
    shift = pno_energy[:, :, None] + pno_energy[:, None, :] - occ_pair[:, None, None]
    signs = jnp.array([1.0, -1.0], jnp.float32)
    factor = shift[:, None, :, :] - signs[None, :, None, None] * frequency[0]
    diagonal_term = factor * amplitudes.astype(jnp.float32)
    return drive + diagonal_term.reshape(PAIRS, 2, R * R) + coupled.reshape(PAIRS, 2, R * R)
```

```python
import jax
import jax.numpy as jnp
from jax import lax
from jax.sharding import PartitionSpec as P


def pair_weights(pair_lmo, neighbours, fock_off, first_pair):
    local_pairs = neighbours.shape[0]
    total_pairs = pair_lmo.shape[0]
    lmo_count = fock_off.shape[0]
    lmo_ids = jnp.arange(lmo_count, dtype=jnp.int32)
    own_lmo = lax.dynamic_slice_in_dim(pair_lmo, first_pair, local_pairs, 0)
    own_table = (own_lmo[:, :, None] == lmo_ids[None, None, :]).astype(jnp.float32)
    lmo_table = (pair_lmo[:, :, None] == lmo_ids[None, None, :]).astype(jnp.float32)
    pair_ids = jnp.arange(total_pairs, dtype=jnp.int32)
    onehot = (neighbours[:, :, None] == pair_ids[None, None, :]).astype(jnp.float32)
    fock_rows = jnp.einsum("psl,lm->psm", own_table, fock_off, precision=lax.Precision.HIGHEST)
    near_table = jnp.einsum("pkn,nsl->pksl", onehot, lmo_table)
    values = jnp.sum(fock_rows[:, None, :, :] * near_table, axis=(2, 3))
    weights = jnp.sum(values[:, :, None] * onehot, axis=1).astype(jnp.bfloat16)
    return (weights, own_table)


def body(
    panels,
    amplitudes,
    drive,
    pno_energy,
    occ_energy,
    frequency,
    pair_lmo,
    neighbours,
    pno_ranks,
    fock_off,
):
    local_pairs, rank_dim, aux_width = panels.shape
    total_pairs = pair_lmo.shape[0]
    n_pair = lax.axis_size("pair")
    n_aux = lax.axis_size("aux")
    first_pair = lax.axis_index("pair") * local_pairs
    rows_index = jnp.arange(rank_dim, dtype=jnp.int32)
    keep_rows = rows_index[None, :] < pno_ranks[:, None]
    weights, own_table = pair_weights(pair_lmo, neighbours, fock_off, first_pair)
    weights = lax.all_gather(weights, "pair", axis=0, tiled=True)
    amps = jnp.where(keep_rows[:, :, None, None], jnp.transpose(amplitudes, (0, 2, 1, 3)), 0)
    amps = lax.all_gather(
        amps.reshape(local_pairs * rank_dim, 2 * rank_dim), "pair", axis=0, tiled=True
    )
    masked = jnp.where(keep_rows[:, :, None], panels, jnp.zeros_like(panels))
    slices = lax.all_to_all(
        masked.reshape(local_pairs * rank_dim, aux_width), "pair", 1, 0, tiled=True
    )
    products = jnp.einsum("iq,jq->ij", slices, slices, preferred_element_type=jnp.float32)
    products = products.reshape(total_pairs, rank_dim, total_pairs, rank_dim)
    mixed = (products * weights.astype(jnp.float32)[:, None, :, None]).astype(jnp.bfloat16)
    mixed = mixed.reshape(total_pairs * rank_dim, total_pairs * rank_dim)
    coupled = jnp.dot(mixed, amps, preferred_element_type=jnp.float32).astype(jnp.bfloat16)
    share_width = drive.shape[2]
    coupled = coupled.reshape(total_pairs, rank_dim, 2, rank_dim).transpose(0, 2, 1, 3)
    coupled = coupled.reshape(n_pair, local_pairs, 2, n_aux, share_width).transpose(0, 3, 1, 2, 4)
    coupled = coupled.reshape(n_pair * n_aux, local_pairs, 2, share_width)
    coupled = lax.all_to_all(coupled, ("pair", "aux"), 0, 0, tiled=True)
    coupled_share = jnp.sum(coupled.astype(jnp.float32), axis=0)
    share_start = lax.axis_index("aux") * share_width
    occ_pair = jnp.sum(own_table * occ_energy[None, None, :], axis=(1, 2))
    shift = pno_energy[:, :, None] + pno_energy[:, None, :] - occ_pair[:, None, None]
    shift_flat = lax.dynamic_slice_in_dim(
        shift.reshape(local_pairs, rank_dim * rank_dim), share_start, share_width, 1
    )
    signs = jnp.array([1.0, -1.0], jnp.float32)
    factor = shift_flat[:, None, :] - signs[None, :, None] * frequency[0]
    amp_flat = amplitudes.reshape(local_pairs, 2, rank_dim * rank_dim)
    amp_share = lax.dynamic_slice_in_dim(amp_flat, share_start, share_width, 2).astype(jnp.float32)
    return drive + factor * amp_share + coupled_share


def solution(mesh):
    placed = (
        P("pair", None, "aux"),
        P("pair", None, None, None),
        P("pair", None, "aux"),
        P("pair", None),
        P(),
        P(),
        P(),
        P("pair", None),
        P("pair"),
        P(),
    )
    return jax.shard_map(
        body, mesh=mesh, in_specs=placed, out_specs=P("pair", None, "aux"), check_vma=False
    )
```

```python
import functools

import jax
import jax.numpy as jnp
from jax import lax
from jax.experimental import pallas as pl
from jax.experimental.pallas import tpu as pltpu
from jax.sharding import PartitionSpec as P

LANE = 128


def pair_weights(pair_lmo, neighbours, fock_off, first_pair):
    local_pairs = neighbours.shape[0]
    total_pairs = pair_lmo.shape[0]
    lmo_count = fock_off.shape[0]
    lmo_ids = jnp.arange(lmo_count, dtype=jnp.int32)
    own_lmo = lax.dynamic_slice_in_dim(pair_lmo, first_pair, local_pairs, 0)
    own_table = (own_lmo[:, :, None] == lmo_ids[None, None, :]).astype(jnp.float32)
    lmo_table = (pair_lmo[:, :, None] == lmo_ids[None, None, :]).astype(jnp.float32)
    pair_ids = jnp.arange(total_pairs, dtype=jnp.int32)
    onehot = (neighbours[:, :, None] == pair_ids[None, None, :]).astype(jnp.float32)
    fock_rows = jnp.einsum("psl,lm->psm", own_table, fock_off, precision=lax.Precision.HIGHEST)
    near_table = jnp.einsum("pkn,nsl->pksl", onehot, lmo_table)
    values = jnp.sum(fock_rows[:, None, :, :] * near_table, axis=(2, 3))
    weights = jnp.sum(values[:, :, None] * onehot, axis=1).astype(jnp.bfloat16)
    return (weights, own_table)


def plain_body(
    panels,
    amplitudes,
    drive,
    pno_energy,
    occ_energy,
    frequency,
    pair_lmo,
    neighbours,
    pno_ranks,
    fock_off,
):
    local_pairs, rank_dim, aux_width = panels.shape
    total_pairs = pair_lmo.shape[0]
    n_pair = lax.axis_size("pair")
    n_aux = lax.axis_size("aux")
    first_pair = lax.axis_index("pair") * local_pairs
    rows_index = jnp.arange(rank_dim, dtype=jnp.int32)
    keep_rows = rows_index[None, :] < pno_ranks[:, None]
    weights, own_table = pair_weights(pair_lmo, neighbours, fock_off, first_pair)
    weights = lax.all_gather(weights, "pair", axis=0, tiled=True)
    amps = jnp.where(keep_rows[:, :, None, None], jnp.transpose(amplitudes, (0, 2, 1, 3)), 0)
    amps = lax.all_gather(
        amps.reshape(local_pairs * rank_dim, 2 * rank_dim), "pair", axis=0, tiled=True
    )
    masked = jnp.where(keep_rows[:, :, None], panels, jnp.zeros_like(panels))
    slices = lax.all_to_all(
        masked.reshape(local_pairs * rank_dim, aux_width), "pair", 1, 0, tiled=True
    )
    products = jnp.einsum("iq,jq->ij", slices, slices, preferred_element_type=jnp.float32)
    products = products.reshape(total_pairs, rank_dim, total_pairs, rank_dim)
    mixed = (products * weights.astype(jnp.float32)[:, None, :, None]).astype(jnp.bfloat16)
    mixed = mixed.reshape(total_pairs * rank_dim, total_pairs * rank_dim)
    coupled = jnp.dot(mixed, amps, preferred_element_type=jnp.float32).astype(jnp.bfloat16)
    share_width = drive.shape[2]
    coupled = coupled.reshape(total_pairs, rank_dim, 2, rank_dim).transpose(0, 2, 1, 3)
    coupled = coupled.reshape(n_pair, local_pairs, 2, n_aux, share_width).transpose(0, 3, 1, 2, 4)
    coupled = coupled.reshape(n_pair * n_aux, local_pairs, 2, share_width)
    coupled = lax.all_to_all(coupled, ("pair", "aux"), 0, 0, tiled=True)
    coupled_share = jnp.sum(coupled.astype(jnp.float32), axis=0)
    share_start = lax.axis_index("aux") * share_width
    occ_pair = jnp.sum(own_table * occ_energy[None, None, :], axis=(1, 2))
    shift = pno_energy[:, :, None] + pno_energy[:, None, :] - occ_pair[:, None, None]
    shift_flat = lax.dynamic_slice_in_dim(
        shift.reshape(local_pairs, rank_dim * rank_dim), share_start, share_width, 1
    )
    signs = jnp.array([1.0, -1.0], jnp.float32)
    factor = shift_flat[:, None, :] - signs[None, :, None] * frequency[0]
    amp_flat = amplitudes.reshape(local_pairs, 2, rank_dim * rank_dim)
    amp_share = lax.dynamic_slice_in_dim(amp_flat, share_start, share_width, 2).astype(jnp.float32)
    return drive + factor * amp_share + coupled_share


def remote(src, dst, send_sem, recv_sem, pair, aux):
    return pltpu.make_async_remote_copy(
        src_ref=src,
        dst_ref=dst,
        send_sem=send_sem,
        recv_sem=recv_sem,
        device_id=(pair, aux),
        device_id_type=pl.DeviceIdType.MESH,
    )


def kernel(
    n_pair, n_aux, rank, x_ref, a_ref, w_ref, out_ref,
    xb, ab, wb, left_rows, acc, parts, parts_in, sums, sums_in,
    local_sem, x_send, x_recv, e_send, e_recv, f_send, f_recv, g_send, g_recv,
    a_send, a_recv, b_send, b_recv, w_send, w_recv, y_send, y_recv, z_send, z_recv,
):
    me = lax.axis_index("pair")
    aux = lax.axis_index("aux")
    core = lax.rem(aux, 2)
    chip = aux // 2
    mate = aux + 1 - 2 * core
    n_chip = n_aux // 2
    block = 2 * rank
    tiles = x_ref.shape[1] // LANE
    base = (tiles // n_pair) * LANE
    extra = tiles % n_pair
    stride = n_pair // (2 * extra) if extra else 1
    share = a_ref.shape[0] // n_aux
    quarter = rank // n_aux
    padded = parts.shape[2] // 2

    barrier = pltpu.get_barrier_semaphore()

    def greet(pair, other):
        pl.semaphore_signal(
            barrier, inc=1, device_id=(pair, other), device_id_type=pl.DeviceIdType.MESH
        )

    for t in range(1, n_pair):
        peer = lax.rem(me + t, n_pair)
        greet(peer, aux)
        greet(peer, mate)
    for t in range(1, n_aux):
        greet(me, lax.rem(aux + t, n_aux))
    pl.semaphore_wait(barrier, 2 * (n_pair - 1) + n_aux - 1)

    def holder(which, level):
        spot = 2 * level + which
        shift = spot % 2 if not hasattr(spot, "dtype") else lax.rem(spot, 2)
        return stride * spot + (shift if stride > 1 else 0)

    lanes = pl.ds(pl.multiple_of(core * base, LANE), base)
    mate_lanes = pl.ds(pl.multiple_of((1 - core) * base, LANE), base)
    extra_lanes = pl.ds(2 * base, LANE)
    my_share = pl.ds(pl.multiple_of(aux * share, 16), share)

    def own_cols(peer):
        return x_ref.at[:, pl.ds(pl.multiple_of(peer * base, LANE), base)]

    def send_a(t):
        peer = lax.rem(me + t, n_pair)
        return remote(a_ref.at[my_share], ab.at[me, my_share], a_send.at[t], a_recv.at[me], peer, aux)

    def send_w(t):
        peer = lax.rem(me + t, n_pair)
        return remote(w_ref, wb.at[me], w_send.at[t], w_recv.at[me], peer, aux)

    def send_x(t):
        peer = lax.rem(me + t, n_pair)
        return remote(own_cols(peer), xb.at[me, :, lanes], x_send.at[t], x_recv.at[me], peer, aux)

    def extra_cols(level):
        return x_ref.at[:, pl.ds(base * n_pair + level * LANE, LANE)]

    def send_e(level):
        return remote(
            extra_cols(level), xb.at[me, :, extra_lanes], e_send.at[level], e_recv.at[me],
            holder(core, level), aux,
        )

    def send_f(j):
        return remote(xb.at[j, :, lanes], xb.at[j, :, lanes], f_send.at[j], f_recv.at[j], me, mate)

    def own_f():
        return remote(own_cols(me), xb.at[me, :, lanes], f_send.at[me], f_recv.at[me], me, mate)

    def send_g(j):
        return remote(
            xb.at[j, :, extra_lanes], xb.at[j, :, extra_lanes], g_send.at[j], g_recv.at[j], me, mate
        )

    def send_b(j, u):
        rows = ab.at[j, my_share]
        return remote(rows, rows, b_send.at[j, u], b_recv.at[aux, j], me, lax.rem(aux + u, n_aux))

    mine_x = pltpu.make_async_copy(own_cols(me), xb.at[me, :, lanes], local_sem.at[0])
    mine_a = pltpu.make_async_copy(a_ref, ab.at[me], local_sem.at[1])
    mine_w = pltpu.make_async_copy(w_ref, wb.at[me], local_sem.at[2])
    for t in range(1, n_pair):
        send_a(t).start()
    for t in range(1, n_pair):
        send_w(t).start()
    order = sorted(range(1, n_pair), key=lambda t: abs(n_pair // 2 - t))
    for t in order:
        send_x(t).start()
    for level in range(extra):
        @pl.when(holder(core, level) != me)
        def _():
            send_e(level).start()

        @pl.when(holder(core, level) == me)
        def _():
            pltpu.make_async_copy(
                extra_cols(level), xb.at[me, :, extra_lanes], local_sem.at[3]
            ).start()
    own_f().start()
    mine_x.start()
    mine_a.start()
    mine_w.start()
    acc[...] = jnp.zeros_like(acc)

    def holds(which):
        found = me < 0
        for level in range(extra):
            found = jnp.logical_or(found, holder(which, level) == me)
        return found

    self_holds = holds(core)
    mate_holds = holds(1 - core)
    if extra:
        @pl.when(jnp.logical_not(jnp.logical_or(self_holds, mate_holds)))
        def _():
            xb[:, :, 2 * base :] = jnp.zeros((n_pair, block, LANE), xb.dtype)

    for t in range(1, n_pair):
        j = lax.rem(me + n_pair - t, n_pair)
        remote(
            a_ref.at[my_share], ab.at[j, my_share], a_send.at[t], a_recv.at[j], me, mate
        ).wait_recv()
        for u in range(1, n_aux):
            send_b(j, u).start()
    for t in order:
        j = lax.rem(me + n_pair - t, n_pair)
        remote(
            own_cols(me), xb.at[j, :, lanes], x_send.at[t], x_recv.at[j], me, mate
        ).wait_recv()
        send_f(j).start()
    mine_x.wait()
    mine_a.wait()
    mine_w.wait()
    if extra:
        @pl.when(self_holds)
        def _():
            pltpu.make_async_copy(
                extra_cols(0), xb.at[me, :, extra_lanes], local_sem.at[3]
            ).wait()
            send_g(me).start()
            for t in range(1, n_pair):
                j = lax.rem(me + n_pair - t, n_pair)
                remote(
                    extra_cols(0), xb.at[j, :, extra_lanes], e_send.at[0], e_recv.at[j], me, mate
                ).wait_recv()
                send_g(j).start()

        @pl.when(mate_holds)
        def _():
            for j in range(n_pair):
                send_g(j).wait_recv()
    for j in range(n_pair):
        remote(
            own_cols(me), xb.at[j, :, mate_lanes], f_send.at[j], f_recv.at[j], me, mate
        ).wait_recv()
    for t in range(1, n_pair):
        j = lax.rem(me + n_pair - t, n_pair)
        remote(w_ref, wb.at[j], w_send.at[t], w_recv.at[j], me, mate).wait_recv()
        for u in range(1, n_aux):
            other = lax.rem(aux + u, n_aux)
            rows = ab.at[j, pl.ds(pl.multiple_of(other * share, 16), share)]
            remote(rows, rows, b_send.at[j, u], b_recv.at[other, j], me, other).wait_recv()

    for half in range(2):
        @pl.when(core == half)
        def _():
            for i in range(n_pair):
                left_rows[pl.ds(i * rank, rank), :] = xb[i, half * rank : (half + 1) * rank, :]

    def couple(j, carry):
        products = lax.dot_general(
            left_rows[...], xb[j], (((1,), (1,)), ((), ())), preferred_element_type=jnp.float32
        )
        scaled = [
            products[i * rank : (i + 1) * rank] * wb[i, core, pl.ds(j, 1), :]
            for i in range(n_pair)
        ]
        mixed = jnp.concatenate(scaled, axis=0).astype(jnp.bfloat16)
        turn = jnp.dot(mixed, ab[j, :block, :], preferred_element_type=jnp.float32)
        for i in range(n_pair):
            acc[i, :rank, :] += turn[i * rank : (i + 1) * rank]
        return carry

    lax.fori_loop(0, n_pair, couple, 0)

    def send_y(i, u):
        other = lax.rem(chip + u, n_chip)
        return remote(
            parts.at[other, i], parts_in.at[u, i], y_send.at[u, i], y_recv.at[u, i],
            me, 2 * other + core,
        )

    def spread(t, carry):
        i = lax.rem(me + 1 + t, n_pair)
        for k in range(n_aux):
            rows = acc[i, pl.ds(quarter * k, padded), :]
            parts[k // 2, i, pl.ds((k % 2) * padded, padded), :] = rows.astype(parts.dtype)
        for u in range(1, n_chip):
            send_y(i, u).start()
        return carry

    lax.fori_loop(0, n_pair, spread, 0)

    def send_z(i, to_core):
        return remote(
            sums.at[i, pl.ds(pl.multiple_of(to_core * padded, padded), padded)],
            sums_in.at[me, core], z_send.at[i, to_core], z_recv.at[me, core],
            i, 2 * chip + to_core,
        )

    def gather_sum(t, carry):
        i = lax.rem(me + 1 + t, n_pair)
        total = parts[chip, i].astype(jnp.float32)
        for u in range(1, n_chip):
            send_y(i, u).wait_recv()
            total = total + parts_in[u, i].astype(jnp.float32)
        sums[i] = total.astype(sums.dtype)

        @pl.when(i != me)
        def _():
            send_z(i, core).start()

        send_z(i, 1 - core).start()
        return carry

    lax.fori_loop(0, n_pair, gather_sum, 0)
    sums_in[me, core] = sums[me, pl.ds(pl.multiple_of(core * padded, padded), padded), :]

    def arrive(j, from_core):
        remote(
            sums.at[j, pl.ds(0, padded)], sums_in.at[j, from_core],
            z_send.at[j, 0], z_recv.at[j, from_core], me, mate,
        ).wait_recv()

    for t in range(n_pair):
        j = lax.rem(me + n_pair - t, n_pair)
        if t:
            arrive(j, core)
        arrive(j, 1 - core)
    for half in range(2):
        total = sums_in[0, half].astype(jnp.float32)
        for j in range(1, n_pair):
            total = total + sums_in[j, half].astype(jnp.float32)
        out_ref[half] = total

    for t in range(1, n_pair):
        send_a(t).wait_send()
        send_w(t).wait_send()
        send_x(t).wait_send()
        j = lax.rem(me + n_pair - t, n_pair)
        send_f(j).wait_send()
        for u in range(1, n_aux):
            send_b(j, u).wait_send()
    own_f().wait_send()
    for level in range(extra):
        @pl.when(holder(core, level) != me)
        def _():
            send_e(level).wait_send()
    if extra:
        @pl.when(self_holds)
        def _():
            for j in range(n_pair):
                send_g(j).wait_send()

    def drain(i, carry):
        for u in range(1, n_chip):
            send_y(i, u).wait_send()

        @pl.when(i != me)
        def _():
            send_z(i, core).wait_send()

        send_z(i, 1 - core).wait_send()
        return carry

    lax.fori_loop(0, n_pair, drain, 0)


def fused_coupling(x_own, a_own, w_own, n_pair, n_aux, rank):
    block = 2 * rank
    tiles = x_own.shape[1] // LANE
    depth = 2 * (tiles // n_pair) * LANE + (LANE if tiles % n_pair else 0)
    n_chip = n_aux // 2
    extra = max(tiles % n_pair, 1)
    padded = -(-(rank // n_aux) // 16) * 16
    tall = -(-(rank - rank // n_aux + padded) // 8) * 8
    dma = pltpu.SemaphoreType.DMA
    bf16 = jnp.bfloat16
    return pl.pallas_call(
        functools.partial(kernel, n_pair, n_aux, rank),
        out_shape=jax.ShapeDtypeStruct((2, padded, block), jnp.float32),
        in_specs=[pl.BlockSpec(memory_space=pltpu.VMEM)] * 3,
        out_specs=pl.BlockSpec(memory_space=pltpu.VMEM),
        scratch_shapes=[
            pltpu.VMEM((n_pair, block, depth), bf16),
            pltpu.VMEM((n_pair,) + a_own.shape, bf16),
            pltpu.VMEM((n_pair,) + w_own.shape, jnp.float32),
            pltpu.VMEM((n_pair * rank, depth), bf16),
            pltpu.VMEM((n_pair, tall, block), jnp.float32),
            pltpu.VMEM((n_chip, n_pair, 2 * padded, block), bf16),
            pltpu.VMEM((n_chip, n_pair, 2 * padded, block), bf16),
            pltpu.VMEM((n_pair, 2 * padded, block), bf16),
            pltpu.VMEM((n_pair, 2, padded, block), bf16),
            dma((4,)),
            dma((n_pair,)), dma((n_pair,)),
            dma((extra,)), dma((n_pair,)),
            dma((n_pair,)), dma((n_pair,)),
            dma((n_pair,)), dma((n_pair,)),
            dma((n_pair,)), dma((n_pair,)),
            dma((n_pair, n_aux)), dma((n_aux, n_pair)),
            dma((n_pair,)), dma((n_pair,)),
            dma((n_chip, n_pair)), dma((n_chip, n_pair)),
            dma((n_pair, 2)), dma((n_pair, 2)),
        ],
        compiler_params=pltpu.CompilerParams(collective_id=0, has_side_effects=True),
    )(x_own, a_own, w_own)


def fits(panels, n_pair, n_aux):
    local_pairs, rank, width = panels.shape
    tiles = width // LANE
    extra = tiles % n_pair
    return (
        local_pairs == 2
        and width % LANE == 0
        and rank % 8 == 0
        and rank % n_aux == 0
        and n_aux % 2 == 0
        and n_pair > 1
        and tiles >= n_pair
        and (extra == 0 or n_pair % (2 * extra) == 0)
    )


def body(*operands):
    if fits(operands[0], lax.axis_size("pair"), lax.axis_size("aux")):
        return kernel_body(*operands)
    return plain_body(*operands)


def kernel_body(
    panels,
    amplitudes,
    drive,
    pno_energy,
    occ_energy,
    frequency,
    pair_lmo,
    neighbours,
    pno_ranks,
    fock_off,
):
    local_pairs, rank_dim, aux_width = panels.shape
    n_pair = lax.axis_size("pair")
    n_aux = lax.axis_size("aux")
    first_pair = lax.axis_index("pair") * local_pairs
    rows_index = jnp.arange(rank_dim, dtype=jnp.int32)
    keep_rows = rows_index[None, :] < pno_ranks[:, None]
    weights, own_table = pair_weights(pair_lmo, neighbours, fock_off, first_pair)
    w_own = jnp.repeat(
        weights.astype(jnp.float32).reshape(local_pairs, n_pair, local_pairs), rank_dim, axis=2
    )
    amps = jnp.where(keep_rows[:, :, None, None], jnp.transpose(amplitudes, (0, 2, 1, 3)), 0)
    amps = amps.reshape(2 * rank_dim, 2 * rank_dim)
    tall = -(-2 * rank_dim // (16 * n_aux)) * 16 * n_aux
    amps = jnp.pad(amps, ((0, tall - 2 * rank_dim), (0, 0)))
    sums = fused_coupling(
        panels.reshape(2 * rank_dim, aux_width), amps, w_own, n_pair, n_aux, rank_dim
    )
    share_width = drive.shape[2]
    quarter = rank_dim // n_aux
    row_start = lax.axis_index("aux") * quarter
    keep_share = lax.dynamic_slice_in_dim(keep_rows, row_start, quarter, 1)
    coupled = sums[:, :quarter].reshape(local_pairs, quarter, 2, rank_dim)
    coupled = jnp.where(keep_share[:, :, None, None], coupled, 0.0).transpose(0, 2, 1, 3)
    occ_pair = jnp.sum(own_table * occ_energy[None, None, :], axis=(1, 2))
    energy_rows = lax.dynamic_slice_in_dim(pno_energy, row_start, quarter, 1)
    shift = energy_rows[:, :, None] + pno_energy[:, None, :] - occ_pair[:, None, None]
    signs = jnp.array([1.0, -1.0], jnp.float32)
    factor = shift[:, None] - signs[None, :, None, None] * frequency[0]
    amp_share = lax.dynamic_slice_in_dim(amplitudes, row_start, quarter, 2).astype(jnp.float32)
    rest = (factor * amp_share + coupled).reshape(local_pairs, 2, share_width)
    return drive + rest


def solution(mesh):
    placed = (
        P("pair", None, "aux"),
        P("pair", None, None, None),
        P("pair", None, "aux"),
        P("pair", None),
        P(),
        P(),
        P(),
        P("pair", None),
        P("pair"),
        P(),
    )
    return jax.shard_map(
        body, mesh=mesh, in_specs=placed, out_specs=P("pair", None, "aux"), check_vma=False
    )
```

```python
import functools

import jax
import jax.numpy as jnp
from jax import lax
from jax.experimental import pallas as pl
from jax.experimental.pallas import tpu as pltpu
from jax.sharding import PartitionSpec as P

LANE = 128


def pair_weights(pair_lmo, neighbours, fock_off, first_pair):
    local_pairs = neighbours.shape[0]
    total_pairs = pair_lmo.shape[0]
    lmo_count = fock_off.shape[0]
    lmo_ids = jnp.arange(lmo_count, dtype=jnp.int32)
    own_lmo = lax.dynamic_slice_in_dim(pair_lmo, first_pair, local_pairs, 0)
    own_table = (own_lmo[:, :, None] == lmo_ids[None, None, :]).astype(jnp.float32)
    lmo_table = (pair_lmo[:, :, None] == lmo_ids[None, None, :]).astype(jnp.float32)
    pair_ids = jnp.arange(total_pairs, dtype=jnp.int32)
    onehot = (neighbours[:, :, None] == pair_ids[None, None, :]).astype(jnp.float32)
    fock_rows = jnp.einsum("psl,lm->psm", own_table, fock_off, precision=lax.Precision.HIGHEST)
    near_table = jnp.einsum("pkn,nsl->pksl", onehot, lmo_table)
    values = jnp.sum(fock_rows[:, None, :, :] * near_table, axis=(2, 3))
    weights = jnp.sum(values[:, :, None] * onehot, axis=1).astype(jnp.bfloat16)
    return (weights, own_table)


def plain_body(
    panels,
    amplitudes,
    drive,
    pno_energy,
    occ_energy,
    frequency,
    pair_lmo,
    neighbours,
    pno_ranks,
    fock_off,
):
    local_pairs, rank_dim, aux_width = panels.shape
    total_pairs = pair_lmo.shape[0]
    n_pair = lax.axis_size("pair")
    n_aux = lax.axis_size("aux")
    first_pair = lax.axis_index("pair") * local_pairs
    rows_index = jnp.arange(rank_dim, dtype=jnp.int32)
    keep_rows = rows_index[None, :] < pno_ranks[:, None]
    weights, own_table = pair_weights(pair_lmo, neighbours, fock_off, first_pair)
    weights = lax.all_gather(weights, "pair", axis=0, tiled=True)
    amps = jnp.where(keep_rows[:, :, None, None], jnp.transpose(amplitudes, (0, 2, 1, 3)), 0)
    amps = lax.all_gather(
        amps.reshape(local_pairs * rank_dim, 2 * rank_dim), "pair", axis=0, tiled=True
    )
    masked = jnp.where(keep_rows[:, :, None], panels, jnp.zeros_like(panels))
    slices = lax.all_to_all(
        masked.reshape(local_pairs * rank_dim, aux_width), "pair", 1, 0, tiled=True
    )
    products = jnp.einsum("iq,jq->ij", slices, slices, preferred_element_type=jnp.float32)
    products = products.reshape(total_pairs, rank_dim, total_pairs, rank_dim)
    mixed = (products * weights.astype(jnp.float32)[:, None, :, None]).astype(jnp.bfloat16)
    mixed = mixed.reshape(total_pairs * rank_dim, total_pairs * rank_dim)
    coupled = jnp.dot(mixed, amps, preferred_element_type=jnp.float32).astype(jnp.bfloat16)
    share_width = drive.shape[2]
    coupled = coupled.reshape(total_pairs, rank_dim, 2, rank_dim).transpose(0, 2, 1, 3)
    coupled = coupled.reshape(n_pair, local_pairs, 2, n_aux, share_width).transpose(0, 3, 1, 2, 4)
    coupled = coupled.reshape(n_pair * n_aux, local_pairs, 2, share_width)
    coupled = lax.all_to_all(coupled, ("pair", "aux"), 0, 0, tiled=True)
    coupled_share = jnp.sum(coupled.astype(jnp.float32), axis=0)
    share_start = lax.axis_index("aux") * share_width
    occ_pair = jnp.sum(own_table * occ_energy[None, None, :], axis=(1, 2))
    shift = pno_energy[:, :, None] + pno_energy[:, None, :] - occ_pair[:, None, None]
    shift_flat = lax.dynamic_slice_in_dim(
        shift.reshape(local_pairs, rank_dim * rank_dim), share_start, share_width, 1
    )
    signs = jnp.array([1.0, -1.0], jnp.float32)
    factor = shift_flat[:, None, :] - signs[None, :, None] * frequency[0]
    amp_flat = amplitudes.reshape(local_pairs, 2, rank_dim * rank_dim)
    amp_share = lax.dynamic_slice_in_dim(amp_flat, share_start, share_width, 2).astype(jnp.float32)
    return drive + factor * amp_share + coupled_share


def remote(src, dst, send_sem, recv_sem, pair, aux):
    return pltpu.make_async_remote_copy(
        src_ref=src,
        dst_ref=dst,
        send_sem=send_sem,
        recv_sem=recv_sem,
        device_id=(pair, aux),
        device_id_type=pl.DeviceIdType.MESH,
    )


def kernel(
    n_pair, n_aux, rank, x_ref, a_ref, w_ref, out_ref,
    xb, ab, wb, wt, left_rows, acc, parts, parts_in, sums, sums_in,
    local_sem, x_send, x_recv, e_send, e_recv, f_send, f_recv, g_send, g_recv,
    a_send, a_recv, b_send, b_recv, w_send, w_recv, y_send, y_recv, z_send, z_recv,
):
    me = lax.axis_index("pair")
    aux = lax.axis_index("aux")
    core = lax.rem(aux, 2)
    chip = aux // 2
    mate = aux + 1 - 2 * core
    n_chip = n_aux // 2
    block = 2 * rank
    tiles = x_ref.shape[1] // LANE
    base = (tiles // n_pair) * LANE
    extra = tiles % n_pair
    stride = n_pair // (2 * extra) if extra else 1
    share = a_ref.shape[0] // n_aux
    quarter = rank // n_aux
    padded = parts.shape[2] // 2

    barrier = pltpu.get_barrier_semaphore()

    def greet(pair, other):
        pl.semaphore_signal(
            barrier, inc=1, device_id=(pair, other), device_id_type=pl.DeviceIdType.MESH
        )

    for t in range(1, n_pair):
        peer = lax.rem(me + t, n_pair)
        greet(peer, aux)
        greet(peer, mate)
    for t in range(1, n_aux):
        greet(me, lax.rem(aux + t, n_aux))
    pl.semaphore_wait(barrier, 2 * (n_pair - 1) + n_aux - 1)

    def holder(which, level):
        spot = 2 * level + which
        shift = spot % 2 if not hasattr(spot, "dtype") else lax.rem(spot, 2)
        return stride * spot + (shift if stride > 1 else 0)

    lanes = pl.ds(pl.multiple_of(core * base, LANE), base)
    mate_lanes = pl.ds(pl.multiple_of((1 - core) * base, LANE), base)
    extra_lanes = pl.ds(2 * base, LANE)
    my_share = pl.ds(pl.multiple_of(aux * share, 16), share)

    def own_cols(peer):
        return x_ref.at[:, pl.ds(pl.multiple_of(peer * base, LANE), base)]

    half = n_pair // 2
    near = (me // half) * half
    far = half - near
    across = lax.rem(me + half, n_pair)

    def near_peer(t):
        return near + lax.rem(me - near + t, half)

    def far_peer(t):
        return far + lax.rem(me - near + t, half)

    def send_a(t):
        peer = near_peer(t) if t else across
        return remote(a_ref.at[my_share], ab.at[me, my_share], a_send.at[t], a_recv.at[me], peer, aux)

    def pass_a(t):
        rows = ab.at[across, my_share]
        return remote(rows, rows, a_send.at[half + t], a_recv.at[across], near_peer(t), aux)

    def wait_a(j):
        remote(
            a_ref.at[my_share], ab.at[j, my_share], a_send.at[0], a_recv.at[j], me, mate
        ).wait_recv()

    def send_w(t):
        peer = lax.rem(me + t, n_pair)
        return remote(w_ref, wb.at[me], w_send.at[t], w_recv.at[me], peer, aux)

    def send_x(peer):
        return remote(
            own_cols(peer), xb.at[me, :, lanes], x_send.at[peer], x_recv.at[me], peer, aux
        )

    def wait_x(j):
        remote(
            own_cols(me), xb.at[j, :, lanes], x_send.at[j], x_recv.at[j], me, mate
        ).wait_recv()

    def wait_f(j):
        remote(
            own_cols(me), xb.at[j, :, mate_lanes], f_send.at[j], f_recv.at[j], me, mate
        ).wait_recv()

    def extra_cols(level):
        return x_ref.at[:, pl.ds(base * n_pair + level * LANE, LANE)]

    def send_e(level):
        return remote(
            extra_cols(level), xb.at[me, :, extra_lanes], e_send.at[level], e_recv.at[me],
            holder(core, level), aux,
        )

    def send_f(j):
        return remote(xb.at[j, :, lanes], xb.at[j, :, lanes], f_send.at[j], f_recv.at[j], me, mate)

    def own_f():
        return remote(own_cols(me), xb.at[me, :, lanes], f_send.at[me], f_recv.at[me], me, mate)

    def send_g(j):
        return remote(
            xb.at[j, :, extra_lanes], xb.at[j, :, extra_lanes], g_send.at[j], g_recv.at[j], me, mate
        )

    def send_b(j, u):
        rows = ab.at[j, my_share]
        return remote(rows, rows, b_send.at[j, u], b_recv.at[aux, j], me, lax.rem(aux + u, n_aux))

    mine_x = pltpu.make_async_copy(own_cols(me), xb.at[me, :, lanes], local_sem.at[0])
    mine_a = pltpu.make_async_copy(a_ref, ab.at[me], local_sem.at[1])
    mine_w = pltpu.make_async_copy(w_ref, wb.at[me], local_sem.at[2])
    for t in range(half):
        send_a(t).start()
    for t in range(1, n_pair):
        send_w(t).start()
    for level in range(extra):
        @pl.when(holder(core, level) != me)
        def _():
            send_e(level).start()

        @pl.when(holder(core, level) == me)
        def _():
            pltpu.make_async_copy(
                extra_cols(level), xb.at[me, :, extra_lanes], local_sem.at[3]
            ).start()
    for t in range(half):
        send_x(far_peer(t)).start()
    own_f().start()
    mine_x.start()
    mine_a.start()
    mine_w.start()
    acc[...] = jnp.zeros_like(acc)

    def holds(which):
        found = me < 0
        for level in range(extra):
            found = jnp.logical_or(found, holder(which, level) == me)
        return found

    self_holds = holds(core)
    mate_holds = holds(1 - core)
    if extra:
        @pl.when(jnp.logical_not(jnp.logical_or(self_holds, mate_holds)))
        def _():
            xb[:, :, 2 * base :] = jnp.zeros((n_pair, block, LANE), xb.dtype)

    wait_a(across)
    for t in range(1, half):
        pass_a(t).start()
    for t in range(1, half):
        send_x(near_peer(t)).start()
    for t in range(half):
        arrived = [far_peer(t)] if t == 0 else [near_peer(half - t), far_peer(half - t)]
        for j in arrived:
            if t:
                wait_a(j)
            for u in range(1, n_aux):
                send_b(j, u).start()
    mine_x.wait()
    mine_a.wait()
    mine_w.wait()
    if extra:
        @pl.when(self_holds)
        def _():
            pltpu.make_async_copy(
                extra_cols(0), xb.at[me, :, extra_lanes], local_sem.at[3]
            ).wait()
            send_g(me).start()
            for t in range(1, n_pair):
                j = lax.rem(me + n_pair - t, n_pair)
                remote(
                    extra_cols(0), xb.at[j, :, extra_lanes], e_send.at[0], e_recv.at[j], me, mate
                ).wait_recv()
                send_g(j).start()

        @pl.when(mate_holds)
        def _():
            for j in range(n_pair):
                send_g(j).wait_recv()
    for t in range(1, half):
        j = near_peer(half - t)
        wait_x(j)
        send_f(j).start()
    for t in range(1, n_pair):
        j = lax.rem(me + n_pair - t, n_pair)
        remote(w_ref, wb.at[j], w_send.at[t], w_recv.at[j], me, mate).wait_recv()
        for u in range(1, n_aux):
            other = lax.rem(aux + u, n_aux)
            rows = ab.at[j, pl.ds(pl.multiple_of(other * share, 16), share)]
            remote(rows, rows, b_send.at[j, u], b_recv.at[other, j], me, other).wait_recv()
    table = wb[...]
    table = jnp.where(core == 0, table[:, 0], table[:, 1]).astype(jnp.bfloat16)
    pair_row = lax.broadcasted_iota(jnp.int32, (LANE, block), 0)
    column = lax.broadcasted_iota(jnp.int32, (LANE, block), 1)
    for j in range(n_pair):
        pick = pair_row == jnp.where(column < rank, 2 * j, 2 * j + 1)
        pick = jnp.where(pick, 1.0, 0.0).astype(jnp.bfloat16)
        wt[j] = jnp.dot(table, pick, preferred_element_type=jnp.float32)

    def collect_rows(start):
        for side in range(2):
            @pl.when(core == side)
            def _():
                for i in range(half):
                    left_rows[start + i] = xb[start + i, side * rank : (side + 1) * rank, :]

    def couple(start, j):
        rows = jnp.concatenate([left_rows[start + i] for i in range(half)], axis=0)
        products = lax.dot_general(
            rows, xb[j], (((1,), (1,)), ((), ())), preferred_element_type=jnp.float32
        )
        scaled = [
            products[i * rank : (i + 1) * rank] * wt[j, pl.ds(start + i, 1), :]
            for i in range(half)
        ]
        mixed = jnp.concatenate(scaled, axis=0).astype(jnp.bfloat16)
        turn = jnp.dot(mixed, ab[j, :block, :], preferred_element_type=jnp.float32)
        for i in range(half):
            acc[start + i, :rank, :] += turn[i * rank : (i + 1) * rank]

    for t in range(half):
        wait_f(near_peer(t))
    collect_rows(near)

    def near_near(t, carry):
        couple(near, near + t)
        return carry

    lax.fori_loop(0, half, near_near, 0)

    def near_far(t, carry):
        j = far_peer(lax.rem(half - t, half))
        wait_x(j)
        send_f(j).start()
        wait_f(j)
        couple(near, j)
        return carry

    lax.fori_loop(0, half, near_far, 0)

    def far_all(j, carry):
        couple(far, j)
        return carry

    def send_y(i, u):
        other = lax.rem(chip + u, n_chip)
        return remote(
            parts.at[other, i], parts_in.at[u, i], y_send.at[u, i], y_recv.at[u, i],
            me, 2 * other + core,
        )

    def turn_pair(t):
        side = jnp.where(t < half, near, far)
        return side + lax.rem(me - near + 1 + t, half)

    def spread(t, carry):
        i = turn_pair(t)
        for k in range(n_aux):
            rows = acc[i, pl.ds(quarter * k, padded), :]
            parts[k // 2, i, pl.ds((k % 2) * padded, padded), :] = rows.astype(parts.dtype)
        for u in range(1, n_chip):
            send_y(i, u).start()
        return carry

    lax.fori_loop(0, half, spread, 0)
    collect_rows(far)
    lax.fori_loop(0, n_pair, far_all, 0)
    lax.fori_loop(half, n_pair, spread, 0)

    def send_z(i, to_core):
        return remote(
            sums.at[i, pl.ds(pl.multiple_of(to_core * padded, padded), padded)],
            sums_in.at[me, core], z_send.at[i, to_core], z_recv.at[me, core],
            i, 2 * chip + to_core,
        )

    def gather_sum(t, carry):
        i = turn_pair(t)
        total = parts[chip, i].astype(jnp.float32)
        for u in range(1, n_chip):
            send_y(i, u).wait_recv()
            total = total + parts_in[u, i].astype(jnp.float32)
        sums[i] = total.astype(sums.dtype)

        @pl.when(i != me)
        def _():
            send_z(i, core).start()

        send_z(i, 1 - core).start()
        return carry

    lax.fori_loop(0, n_pair, gather_sum, 0)
    sums_in[me, core] = sums[me, pl.ds(pl.multiple_of(core * padded, padded), padded), :]

    def arrive(j, from_core):
        remote(
            sums.at[j, pl.ds(0, padded)], sums_in.at[j, from_core],
            z_send.at[j, 0], z_recv.at[j, from_core], me, mate,
        ).wait_recv()

    for t in range(n_pair):
        j = lax.rem(me + n_pair - t, n_pair)
        if t:
            arrive(j, core)
        arrive(j, 1 - core)
    for side in range(2):
        total = sums_in[0, side].astype(jnp.float32)
        for j in range(1, n_pair):
            total = total + sums_in[j, side].astype(jnp.float32)
        out_ref[side] = total

    for t in range(half):
        send_a(t).wait_send()
        send_x(far_peer(t)).wait_send()
        if t:
            pass_a(t).wait_send()
            send_x(near_peer(t)).wait_send()
    for t in range(1, n_pair):
        send_w(t).wait_send()
        j = lax.rem(me + n_pair - t, n_pair)
        send_f(j).wait_send()
        for u in range(1, n_aux):
            send_b(j, u).wait_send()
    own_f().wait_send()
    for level in range(extra):
        @pl.when(holder(core, level) != me)
        def _():
            send_e(level).wait_send()
    if extra:
        @pl.when(self_holds)
        def _():
            for j in range(n_pair):
                send_g(j).wait_send()

    def drain(i, carry):
        for u in range(1, n_chip):
            send_y(i, u).wait_send()

        @pl.when(i != me)
        def _():
            send_z(i, core).wait_send()

        send_z(i, 1 - core).wait_send()
        return carry

    lax.fori_loop(0, n_pair, drain, 0)


def fused_coupling(x_own, a_own, w_own, n_pair, n_aux, rank):
    block = 2 * rank
    tiles = x_own.shape[1] // LANE
    depth = 2 * (tiles // n_pair) * LANE + (LANE if tiles % n_pair else 0)
    n_chip = n_aux // 2
    extra = max(tiles % n_pair, 1)
    padded = -(-(rank // n_aux) // 16) * 16
    tall = -(-(rank - rank // n_aux + padded) // 8) * 8
    dma = pltpu.SemaphoreType.DMA
    bf16 = jnp.bfloat16
    return pl.pallas_call(
        functools.partial(kernel, n_pair, n_aux, rank),
        out_shape=jax.ShapeDtypeStruct((2, padded, block), jnp.float32),
        in_specs=[pl.BlockSpec(memory_space=pltpu.VMEM)] * 3,
        out_specs=pl.BlockSpec(memory_space=pltpu.VMEM),
        scratch_shapes=[
            pltpu.VMEM((n_pair, block, depth), bf16),
            pltpu.VMEM((n_pair,) + a_own.shape, bf16),
            pltpu.VMEM((n_pair,) + w_own.shape, jnp.float32),
            pltpu.VMEM((n_pair, n_pair, block), jnp.float32),
            pltpu.VMEM((n_pair, rank, depth), bf16),
            pltpu.VMEM((n_pair, tall, block), jnp.float32),
            pltpu.VMEM((n_chip, n_pair, 2 * padded, block), bf16),
            pltpu.VMEM((n_chip, n_pair, 2 * padded, block), bf16),
            pltpu.VMEM((n_pair, 2 * padded, block), bf16),
            pltpu.VMEM((n_pair, 2, padded, block), bf16),
            dma((4,)),
            dma((n_pair,)), dma((n_pair,)),
            dma((extra,)), dma((n_pair,)),
            dma((n_pair,)), dma((n_pair,)),
            dma((n_pair,)), dma((n_pair,)),
            dma((n_pair,)), dma((n_pair,)),
            dma((n_pair, n_aux)), dma((n_aux, n_pair)),
            dma((n_pair,)), dma((n_pair,)),
            dma((n_chip, n_pair)), dma((n_chip, n_pair)),
            dma((n_pair, 2)), dma((n_pair, 2)),
        ],
        compiler_params=pltpu.CompilerParams(collective_id=0, has_side_effects=True),
    )(x_own, a_own, w_own)


def fits(panels, n_pair, n_aux):
    local_pairs, rank, width = panels.shape
    tiles = width // LANE
    extra = tiles % n_pair
    return (
        local_pairs == 2
        and width % LANE == 0
        and rank % 8 == 0
        and rank % n_aux == 0
        and n_aux % 2 == 0
        and n_pair % 2 == 0
        and 2 * n_pair <= LANE
        and tiles >= n_pair
        and (extra == 0 or n_pair % (2 * extra) == 0)
    )


def body(*operands):
    if fits(operands[0], lax.axis_size("pair"), lax.axis_size("aux")):
        return kernel_body(*operands)
    return plain_body(*operands)


def kernel_body(
    panels,
    amplitudes,
    drive,
    pno_energy,
    occ_energy,
    frequency,
    pair_lmo,
    neighbours,
    pno_ranks,
    fock_off,
):
    local_pairs, rank_dim, aux_width = panels.shape
    n_pair = lax.axis_size("pair")
    n_aux = lax.axis_size("aux")
    first_pair = lax.axis_index("pair") * local_pairs
    rows_index = jnp.arange(rank_dim, dtype=jnp.int32)
    keep_rows = rows_index[None, :] < pno_ranks[:, None]
    weights, own_table = pair_weights(pair_lmo, neighbours, fock_off, first_pair)
    w_own = jnp.pad(weights.astype(jnp.float32), ((0, 0), (0, LANE - weights.shape[1])))
    amps = jnp.where(keep_rows[:, :, None, None], jnp.transpose(amplitudes, (0, 2, 1, 3)), 0)
    amps = amps.reshape(2 * rank_dim, 2 * rank_dim)
    tall = -(-2 * rank_dim // (16 * n_aux)) * 16 * n_aux
    amps = jnp.pad(amps, ((0, tall - 2 * rank_dim), (0, 0)))
    sums = fused_coupling(
        panels.reshape(2 * rank_dim, aux_width), amps, w_own, n_pair, n_aux, rank_dim
    )
    share_width = drive.shape[2]
    quarter = rank_dim // n_aux
    row_start = lax.axis_index("aux") * quarter
    keep_share = lax.dynamic_slice_in_dim(keep_rows, row_start, quarter, 1)
    coupled = sums[:, :quarter].reshape(local_pairs, quarter, 2, rank_dim)
    coupled = jnp.where(keep_share[:, :, None, None], coupled, 0.0).transpose(0, 2, 1, 3)
    occ_pair = jnp.sum(own_table * occ_energy[None, None, :], axis=(1, 2))
    energy_rows = lax.dynamic_slice_in_dim(pno_energy, row_start, quarter, 1)
    shift = energy_rows[:, :, None] + pno_energy[:, None, :] - occ_pair[:, None, None]
    signs = jnp.array([1.0, -1.0], jnp.float32)
    factor = shift[:, None] - signs[None, :, None, None] * frequency[0]
    amp_share = lax.dynamic_slice_in_dim(amplitudes, row_start, quarter, 2).astype(jnp.float32)
    rest = (factor * amp_share + coupled).reshape(local_pairs, 2, share_width)
    return drive + rest


def solution(mesh):
    placed = (
        P("pair", None, "aux"),
        P("pair", None, None, None),
        P("pair", None, "aux"),
        P("pair", None),
        P(),
        P(),
        P(),
        P("pair", None),
        P("pair"),
        P(),
    )
    return jax.shard_map(
        body, mesh=mesh, in_specs=placed, out_specs=P("pair", None, "aux"), check_vma=False
    )
```
